32 devices in a mesh: lon: 8 (over y, x, core), lat: 4 (over z).
Axes of the slice: x: 2, y: 2, z: 4, core: 2. Of those that a mesh axis runs over, the one named last changes fastest.
Arguments:
- air_state: bfloat16 [4, 24, 192, 192], P(None, 'lat', 'lon'), may hold values from -6 to 6
- upstream: bfloat16 [4, 24, 192, 192], P(None, 'lat', 'lon'), may hold values from -6 to 6
- norm_gain: float32 [192], replicated, may hold values from 0.25 to 1.75
- w_qkv: bfloat16 [192, 576], replicated, may hold values from -0.4375 to 0.4375
- w_proj: bfloat16 [192, 192], replicated, may hold values from -0.4375 to 0.4375
- bias_table: float32 [4, 2, 6, 3312], P('lat'), may hold values from -5 to 260
Outputs:
- block_out: bfloat16 [4, 24, 192, 192], P(None, 'lat', 'lon')
- d_state: bfloat16 [4, 24, 192, 192], P(None, 'lat', 'lon')
- d_gain: float32 [192], replicated
- d_wqkv: float32 [192, 576], replicated
- d_wproj: float32 [192, 192], replicated
- d_table: float32 [4, 2, 6, 3312], P('lat')
The draws below stay inside these ranges and needn't reach their ends.
All inputs are finite; a program needn't handle non-finite values.
Results may differ from the reference program's by a relative error of at most 0.019.
Values may be sent and summed in bfloat16 or wider, within the bound.
A program may use at most 128 MiB of HBM per device.

```python
from functools import partial
import jax
import jax.numpy as jnp
from jax import lax

C = 192
HEADS = 6
WLEV = 2
WLAT = 6
WLON = 12
LEV = 4
WIN = 144
REL = 3312
LEVW = 2
LAT = 24
LON = 192
BANDS = 4


def draw_bias_table(key, part):
    base_key = jax.random.fold_in(key, 11)
    shape = (BANDS, LEVW, HEADS, REL)
    return jnp.clip(jax.random.normal(base_key, shape, jnp.float32), -5.0, 5.0)


def level_of(own_key, shape, pieces, least, largest):
    factor_of, own = 1.0, jax.random.fold_in(own_key, 6)
    for axis_at, parts in pieces:
        steps = jnp.exp(jax.random.uniform(jax.random.fold_in(own, axis_at), (parts,), jnp.float32, least / len(pieces), largest / len(pieces)))
        factor_of = factor_of * jnp.repeat(steps, shape[axis_at] // parts).reshape([-1 if axis == axis_at else 1 for axis in range(len(shape))])
    return factor_of


def bell_draw(key, extent, spread, most, pieces=(), held_as=jnp.bfloat16):
    entries = jax.random.normal(key, extent, jnp.float32) * spread
    if len(pieces) > 0:
        entries = level_of(key, extent, pieces, -0.22, 0.18) * entries
    return jnp.clip(entries, min=-most, max=most).astype(held_as)


def setup_inputs(seed: int = 0) -> dict:
    key_of = jax.random.split(jax.random.key(seed), 7)
    return {
        "air_state": bell_draw(key_of[0], (LEV, LAT, LON, C), 1.0, 6.0, ((1, 4), (2, 8))),
        "upstream": bell_draw(key_of[1], (LEV, LAT, LON, C), 1.0, 6.0, ((1, 4), (2, 8))),
        "norm_gain": jnp.clip(1.0 + 0.15 * jax.random.normal(key_of[2], (C,), jnp.float32), 0.25, 1.75),
        "w_qkv": bell_draw(key_of[3], (C, 3 * C), C ** -0.5, 0.4375),
        "w_proj": bell_draw(key_of[4], (C, C), C ** -0.5, 0.4375),
        "bias_table": draw_bias_table(jax.random.fold_in(key_of[6], 71), 0),
    }


epsilon = 1e-05
masked_score = -1000000000.0

def layer_norm(as_input, gain_vec):
    average = lax.optimization_barrier(jnp.mean(as_input, axis=-1, keepdims=True))
    centred = as_input - average
    variance = lax.optimization_barrier(jnp.mean(centred * centred, axis=-1, keepdims=True))
    return centred * lax.rsqrt(variance + epsilon) * gain_vec

def attention_core(qkv_rows, table_row, first_row, lat_total):
    lev_count, col_count = (qkv_rows.shape[0], qkv_rows.shape[2])
    head_width = qkv_rows.shape[5]
    lev_wins, lon_wins = (lev_count // WLEV, col_count // WLON)
    windowed = qkv_rows.reshape(lev_wins, WLEV, WLAT, lon_wins, WLON, 3, HEADS, head_width)
    windowed = windowed.transpose(5, 0, 3, 6, 1, 2, 4, 7).reshape(3, lev_wins, lon_wins, HEADS, WIN, head_width)
    queries, keyset, values = (windowed[0], windowed[1], windowed[2])
    scores = jnp.einsum('achid,achjd->achij', queries, keyset, preferred_element_type=jnp.float32) * head_width ** (-0.5)
    picked = table_row.reshape(lev_wins, HEADS, WLEV * WLAT, WLEV * WLAT, 2 * WLON - 1)
    offsets = jnp.arange(WLON)
    onehot = (offsets[None, :, None] - offsets[:, None, None] + WLON - 1 == jnp.arange(2 * WLON - 1)[None, None, :]).astype(jnp.float32)
    expanded = jnp.einsum('ahpqr,ijr->ahpiqj', picked, onehot, precision=lax.Precision.HIGHEST)
    expanded = expanded.reshape(lev_wins, 1, HEADS, WIN, WIN)
    scores = scores + expanded
    lev_index = jnp.arange(lev_wins * WLEV).reshape(lev_wins, WLEV)
    lev_part = (lev_index >= lev_count - WLEV // 2).astype(jnp.int32)
    lat_index = first_row + jnp.arange(WLAT, dtype=jnp.int32)
    lat_part = (lat_index >= lat_total - WLAT // 2).astype(jnp.int32)
    region = 2 * lev_part[:, :, None, None] + lat_part[None, None, :, None] + jnp.zeros((1, 1, 1, WLON), jnp.int32)
    region = region.reshape(lev_wins, WIN)
    same_region = region[:, None, None, :, None] == region[:, None, None, None, :]
    scores = jnp.where(same_region, scores, masked_score)
    row_max = lax.stop_gradient(lax.optimization_barrier(jnp.max(scores, axis=-1, keepdims=True)))
    weights = jnp.exp(scores - row_max)
    softened = (weights / lax.optimization_barrier(jnp.sum(weights, axis=-1, keepdims=True))).astype(jnp.bfloat16)
    mixture = jnp.einsum('achij,achjd->achid', softened, values, preferred_element_type=jnp.float32).astype(jnp.bfloat16)
    mixture = mixture.reshape(lev_wins, lon_wins, HEADS, WLEV, WLAT, WLON, head_width)
    return mixture.transpose(0, 3, 4, 1, 5, 2, 6).reshape(lev_count, WLAT, col_count, HEADS * head_width)

def local_sublayer(shifted, shifted_up, gain_vec, w_qkv, w_proj, table_row, first_row, lat_total):
    lev_count, row_count, col_count, width = shifted.shape
    pre_norm, norm_back = jax.vjp(layer_norm, shifted.astype(jnp.float32), gain_vec)
    normed = pre_norm.astype(jnp.bfloat16).reshape(-1, width)
    qkv_rows = jnp.dot(normed, w_qkv, preferred_element_type=jnp.float32).astype(jnp.bfloat16)
    qkv_rows = qkv_rows.reshape(lev_count, row_count, col_count, 3, HEADS, width // HEADS)
    core_fn = partial(attention_core, first_row=first_row, lat_total=lat_total)
    mixture, core_back = jax.vjp(core_fn, qkv_rows, table_row)
    flat_rows = mixture.reshape(-1, width)
    branch = jnp.dot(flat_rows, w_proj, preferred_element_type=jnp.float32).astype(jnp.bfloat16)
    up_rows = shifted_up.reshape(-1, width)
    d_proj = jnp.einsum('ti,to->io', flat_rows, up_rows, preferred_element_type=jnp.float32)
    d_mixed = jnp.einsum('to,io->ti', up_rows, w_proj, preferred_element_type=jnp.float32).astype(jnp.bfloat16)
    d_qkv, d_row = core_back(d_mixed.reshape(mixture.shape))
    d_qkv = d_qkv.reshape(-1, 3 * width)
    d_wqkv = jnp.einsum('ti,to->io', normed, d_qkv, preferred_element_type=jnp.float32)
    d_normed = jnp.einsum('to,io->ti', d_qkv, w_qkv, preferred_element_type=jnp.float32)
    d_input, d_gain = norm_back(d_normed.reshape(lev_count, row_count, col_count, width))
    branch = branch.reshape(lev_count, row_count, col_count, width)
    return (branch, d_input.astype(jnp.bfloat16), d_gain, d_wqkv, d_proj, d_row)

def reference(air_state, upstream, norm_gain, w_qkv, w_proj, bias_table):
    lev_shift, lat_shift, lon_shift = (WLEV // 2, WLAT // 2, WLON // 2)
    rolled = jnp.roll(air_state, (-lev_shift, -lat_shift, -lon_shift), (0, 1, 2))
    rolled_up = jnp.roll(upstream, (-lev_shift, -lat_shift, -lon_shift), (0, 1, 2))
    lat_total = air_state.shape[1]
    width = air_state.shape[3]

    def row_step(totals, window_row):
        first_row = window_row * WLAT
        block_in = lax.dynamic_slice_in_dim(rolled, first_row, WLAT, 1)
        block_up = lax.dynamic_slice_in_dim(rolled_up, first_row, WLAT, 1)
        table_row = lax.dynamic_index_in_dim(bias_table, window_row, 0, keepdims=False)
        results = local_sublayer(block_in, block_up, norm_gain, w_qkv, w_proj, table_row, first_row, lat_total)
        totals = tuple((before + added for before, added in zip(totals, results[2:5])))
        return (totals, (results[0], results[1], results[5]))
    zeros_init = (jnp.zeros((width,), jnp.float32), jnp.zeros((width, 3 * width), jnp.float32), jnp.zeros((width, width), jnp.float32))
    totals, (branches, gradients, d_table) = lax.scan(row_step, zeros_init, jnp.arange(lat_total // WLAT, dtype=jnp.int32))
    shape_out = air_state.shape
    branches = branches.transpose(1, 0, 2, 3, 4).reshape(shape_out)
    gradients = gradients.transpose(1, 0, 2, 3, 4).reshape(shape_out)
    branches = jnp.roll(branches, (lev_shift, lat_shift, lon_shift), (0, 1, 2))
    gradients = jnp.roll(gradients, (lev_shift, lat_shift, lon_shift), (0, 1, 2))
    block_out = (air_state.astype(jnp.float32) + branches.astype(jnp.float32)).astype(jnp.bfloat16)
    d_state = (upstream.astype(jnp.float32) + gradients.astype(jnp.float32)).astype(jnp.bfloat16)
    return (block_out, d_state, totals[0], totals[1], totals[2], d_table)
```

```python
from functools import partial

import jax
import jax.numpy as jnp
from jax import lax
from jax.experimental import pallas as pl
from jax.experimental.pallas import tpu as pltpu
from jax.sharding import PartitionSpec as P

HEADS = 6
WLEV = 2
WLAT = 6
WLON = 12
WIN = 144
PLACES = WLEV * WLAT
OFFS = 2 * WLON - 1
LAT_SHIFT = WLAT // 2
LON_SHIFT = WLON // 2
EDGE = 8

epsilon = 1e-05
masked_score = -1000000000.0
F32 = jnp.float32
BF16 = jnp.bfloat16


def mm(a, b):
    return lax.dot_general(a, b, (((1,), (0,)), ((), ())), preferred_element_type=F32)


def mm_nt(a, b):
    return lax.dot_general(a, b, (((1,), (1,)), ((), ())), preferred_element_type=F32)


def mm_tn(a, b):
    return lax.dot_general(a, b, (((0,), (0,)), ((), ())), preferred_element_type=F32)


def group_of(n):
    return sum((n >= WLON * m).astype(jnp.int32) for m in range(1, PLACES))


def selection(lon_i):
    k = lax.broadcasted_iota(jnp.int32, (PLACES * OFFS, WIN), 0)
    n = lax.broadcasted_iota(jnp.int32, (1, WIN), 1)
    target = n + (OFFS - WLON) * group_of(n) + (WLON - 1) - lon_i
    return jnp.where(k == target, 1.0, 0.0).astype(BF16)


def core_kernel(
    air, up, east, north, corner, gain, w_qkv, w_proj, table,
    out24, out8, grads, d_table,
    x, y, xhat, rstd_s, normed, qkv, d_mix, bias, d_bias, acc_o, acc_dq, acc_dk, acc_dv, dqkv, mix, stage,
):
    lev, rows, cols, width = air.shape
    lev_wins, lon_wins = lev // WLEV, cols // WLON
    wins = lev_wins * lon_wins
    head_width = width // HEADS
    scale = head_width ** (-0.5)

    for src, (dst) in enumerate((x, y)):
        local = (air, up)[src]
        for rl in range(lev):
            a, l = divmod(rl, WLEV)
            ol = (rl + WLEV // 2) % lev
            for t in range(WLAT):
                p = l * WLAT + t
                if t < WLAT - LAT_SHIFT:
                    row = local[ol, t + LAT_SHIFT].astype(F32)
                    edge = east[src, ol, t + LAT_SHIFT].astype(F32)
                else:
                    row = north[src, ol, t - (WLAT - LAT_SHIFT)].astype(F32)
                    edge = corner[src, ol, t - (WLAT - LAT_SHIFT)].astype(F32)
                for c in range(lon_wins):
                    w = a * lon_wins + c
                    lo = LON_SHIFT + c * WLON
                    if c < lon_wins - 1:
                        dst[w, p * WLON:(p + 1) * WLON, :] = row[lo:lo + WLON]
                    else:
                        dst[w, p * WLON:p * WLON + WLON - LON_SHIFT, :] = row[lo:cols]
                        dst[w, p * WLON + WLON - LON_SHIFT:(p + 1) * WLON, :] = edge[:LON_SHIFT]

    t_val = table[...]
    t_hi = t_val.astype(BF16)
    t_rest = t_val - t_hi.astype(F32)
    t_mid = t_rest.astype(BF16)
    t_lo = (t_rest - t_mid.astype(F32)).astype(BF16)
    last_band = lax.axis_index("lat") == lax.axis_size("lat") - 1
    for lon_i in range(WLON):
        sel = selection(lon_i)
        b = mm(t_hi, sel) + mm(t_mid, sel) + mm(t_lo, sel)
        bias[:, lon_i, :] = b

    wq_all = w_qkv[...]
    for w in range(wins):
        xv = x[w]
        mean = jnp.mean(xv, axis=-1, keepdims=True)
        cen = xv - mean
        var = jnp.mean(cen * cen, axis=-1, keepdims=True)
        rs = lax.rsqrt(var + epsilon)
        xh = cen * rs
        xhat[w] = xh
        rstd_s[w] = rs
        nb = (xh * gain[...]).astype(BF16)
        normed[w] = nb
        res = mm(nb, wq_all).astype(BF16)
        for s in range(3):
            qkv[s, w] = res[:, s * width:(s + 1) * width]
        d_mix[w] = mm_nt(y[w].astype(BF16), w_proj[...]).astype(BF16)

    acc_o[...] = jnp.zeros_like(acc_o)
    acc_dq[...] = jnp.zeros_like(acc_dq)
    acc_dk[...] = jnp.zeros_like(acc_dk)
    acc_dv[...] = jnp.zeros_like(acc_dv)

    ri = lax.broadcasted_iota(jnp.int32, (WIN, WIN), 0)
    ci = lax.broadcasted_iota(jnp.int32, (WIN, WIN), 1)
    half = WIN // WLEV
    quarter = LAT_SHIFT * WLON

    def lev_of(n):
        return n >= half

    def lat_of(n):
        return jnp.where(n >= half, n - half, n) >= quarter

    lev_same = jnp.where(lev_of(ri) == lev_of(ci), 1, 0)
    lat_same = jnp.where(lat_of(ri) == lat_of(ci), 1, 0)
    lane = lax.broadcasted_iota(jnp.int32, (WIN, width), 1)

    def head_step(ah, carry):
        a = ah // HEADS
        h = ah - a * HEADS
        keep_lev = jnp.where(a == lev_wins - 1, 0, 1)
        keep_lat = jnp.where(last_band, 0, 1)
        same = ((lev_same + keep_lev) * (lat_same + keep_lat)) > 0
        bias_h = bias[pl.ds(ah * PLACES, PLACES)].reshape(WIN, WIN)
        bias_h = jnp.where(same, bias_h, masked_score)
        head = (lane >= h * head_width) & (lane < (h + 1) * head_width)
        d_bias_h = None
        for c in range(lon_wins):
            w = a * lon_wins + c
            q, k, v, dm = qkv[0, w], qkv[1, w], qkv[2, w], d_mix[w]
            zero = jnp.zeros_like(q)
            qm, km = jnp.where(head, q, zero), jnp.where(head, k, zero)
            vm, dmm = jnp.where(head, v, zero), jnp.where(head, dm, zero)
            s = mm_nt(q, km) * scale + bias_h
            m = jnp.max(s, axis=-1, keepdims=True)
            e = jnp.exp(s - m)
            pf = e / jnp.sum(e, axis=-1, keepdims=True)
            pb = pf.astype(BF16)
            acc_o[w] += mm(pb, vm)
            dp = mm_nt(dm, vm).astype(BF16).astype(F32)
            acc_dv[w] += mm_tn(pb, dmm)
            ds = pf * (dp - jnp.sum(dp * pf, axis=-1, keepdims=True))
            d_bias_h = ds if d_bias_h is None else d_bias_h + ds
            dsb = (ds * scale).astype(BF16)
            acc_dq[w] += mm(dsb, km)
            acc_dk[w] += mm_tn(dsb, qm)
        d_bias[pl.ds(ah * PLACES, PLACES)] = d_bias_h.reshape(PLACES, WLON, WIN)
        return carry

    lax.fori_loop(0, lev_wins * HEADS, head_step, 0)

    total = None
    for lon_i in range(WLON):
        part = mm_nt(d_bias[:, lon_i, :].astype(BF16), selection(lon_i))
        total = part if total is None else total + part
    d_table[...] = total.astype(d_table.dtype)

    stage[...] = jnp.zeros_like(stage)
    d_gain = jnp.zeros((1, width), F32)
    for w in range(wins):
        a, c = divmod(w, lon_wins)
        mb = acc_o[w].astype(BF16)
        mix[w] = mb
        for s, acc in enumerate((acc_dq, acc_dk, acc_dv)):
            dqkv[w, :, s * width:(s + 1) * width] = acc[w].astype(BF16)
        branch = mm(mb, w_proj[...])
        d_pre = mm_nt(dqkv[w], wq_all)
        xh = xhat[w]
        d_gain = d_gain + jnp.sum(d_pre * xh, axis=0, keepdims=True)
        g = d_pre * gain[...]
        dx = rstd_s[w] * (
            g - jnp.mean(g, axis=-1, keepdims=True) - xh * jnp.mean(g * xh, axis=-1, keepdims=True)
        )
        for n, val in enumerate((branch, dx)):
            for p in range(PLACES):
                l, t = divmod(p, WLAT)
                ol = (a * WLEV + l + WLEV // 2) % lev
                lo = LON_SHIFT + c * WLON
                stage[n, ol, t, lo:lo + WLON, :] = val[p * WLON:(p + 1) * WLON]
    out24[...] = stage[:, :, :, 0:cols, :].astype(BF16)
    out8[...] = stage[:, :, :, cols:cols + EDGE, :].astype(BF16)

    dwq = None
    dwp = None
    for w in range(wins):
        one = mm_tn(normed[w], dqkv[w])
        two = mm_tn(mix[w], y[w].astype(BF16))
        dwq = one if dwq is None else dwq + one
        dwp = two if dwp is None else dwp + two
    parts, share, _ = grads.shape
    per = width // parts
    for n in range(parts):
        grads[n, 0:per, 0:3 * width] = dwq[n * per:(n + 1) * per].astype(BF16)
        grads[n, 0:per, 3 * width:4 * width] = dwp[n * per:(n + 1) * per].astype(BF16)
        grads[n, per:share, 0:width] = jnp.broadcast_to(d_gain, (share - per, width)).astype(BF16)
        grads[n, per:share, width:4 * width] = jnp.zeros((share - per, 3 * width), BF16)


def core_call(air, up, east, north, corner, gain, w_qkv, w_proj, table, parts):
    lev, rows, cols, width = air.shape
    wins = (lev // WLEV) * (cols // WLON)
    pairs = (lev // WLEV) * HEADS
    share = width // parts + 8
    vm = lambda shape, dtype: pltpu.VMEM(shape, dtype)
    win_f = vm((wins, WIN, width), F32)
    win_b = vm((wins, WIN, width), BF16)
    spec = pl.BlockSpec(memory_space=pltpu.VMEM)
    return pl.pallas_call(
        core_kernel,
        out_shape=(
            jax.ShapeDtypeStruct((2, lev, rows, cols, width), BF16),
            jax.ShapeDtypeStruct((2, lev, rows, EDGE, width), BF16),
            jax.ShapeDtypeStruct((parts, share, 4 * width), BF16),
            jax.ShapeDtypeStruct(table.shape, BF16),
        ),
        in_specs=[spec] * 9,
        out_specs=(spec,) * 4,
        scratch_shapes=[
            win_f, win_f, win_f,
            vm((wins, WIN, 1), F32),
            win_b,
            vm((3, wins, WIN, width), BF16),
            win_b,
            vm((pairs * PLACES, WLON, WIN), F32),
            vm((pairs * PLACES, WLON, WIN), F32),
            win_f, win_f, win_f, win_f,
            vm((wins, WIN, 3 * width), BF16),
            win_b,
            vm((2, lev, rows, cols + EDGE, width), F32),
        ],
        compiler_params=pltpu.CompilerParams(vmem_limit_bytes=60 * 1024 * 1024),
        name="window_core",
    )(air, up, east, north, corner, gain, w_qkv, w_proj, table)


def from_behind(array, axis, by):
    peers = lax.axis_size(axis)
    return lax.ppermute(array, axis, [(i, (i + by) % peers) for i in range(peers)])


def on_device(air_state, upstream, norm_gain, w_qkv, w_proj, bias_table):
    lev, rows, cols, width = air_state.shape
    parts = lax.axis_size("lon")
    both = jnp.stack([air_state, upstream])
    east = from_behind(both[:, :, :, :EDGE], "lon", -1)
    north = from_behind(both[:, :, :LAT_SHIFT], "lat", -1)
    corner = from_behind(east[:, :, :LAT_SHIFT], "lat", -1)
    pairs = (lev // WLEV) * HEADS
    out24, out8, grads, d_table = core_call(
        air_state, upstream, east, north, corner, norm_gain.reshape(1, width), w_qkv, w_proj,
        bias_table.reshape(pairs * PLACES, PLACES * OFFS), parts,
    )
    keep = WLAT - LAT_SHIFT
    edge_west = from_behind(out8, "lon", 1)
    south24 = from_behind(out24[:, :, keep:], "lat", 1)
    south8 = from_behind(edge_west[:, :, keep:], "lat", 1)
    wide = jnp.concatenate([south24, out24[:, :, :keep]], axis=2)
    edge = jnp.concatenate([south8, edge_west[:, :, :keep]], axis=2)
    edge = jnp.pad(edge, ((0, 0), (0, 0), (0, 0), (0, cols - EDGE), (0, 0)))
    total = both.astype(F32) + wide.astype(F32) + edge.astype(F32)
    total = total.astype(BF16)
    grads = lax.psum(grads, ("lon", "lat")).astype(F32)
    d_table = lax.psum(d_table, "lon").astype(F32)
    per = width // parts
    d_wqkv = grads[:, :per, :3 * width].reshape(width, 3 * width)
    d_wproj = grads[:, :per, 3 * width:].reshape(width, width)
    d_gain = grads[0, per, :width]
    return total[0], total[1], d_gain, d_wqkv, d_wproj, d_table.reshape(bias_table.shape)


def solution(mesh):
    return jax.shard_map(
        on_device,
        mesh=mesh,
        in_specs=(
            P(None, "lat", "lon", None),
            P(None, "lat", "lon", None),
            P(),
            P(),
            P(),
            P("lat", None, None, None),
        ),
        out_specs=(
            P(None, "lat", "lon", None),
            P(None, "lat", "lon", None),
            P(),
            P(),
            P(),
            P("lat", None, None, None),
        ),
        check_vma=False,
    )
```

```python
from functools import partial

import jax
import jax.numpy as jnp
from jax import lax
from jax.experimental import pallas as pl
from jax.experimental.pallas import tpu as pltpu
from jax.sharding import PartitionSpec as P

HEADS = 6
WLEV = 2
WLAT = 6
WLON = 12
WIN = 144
PLACES = WLEV * WLAT
OFFS = 2 * WLON - 1
LAT_SHIFT = WLAT // 2
LON_SHIFT = WLON // 2
EDGE = 8

epsilon = 1e-05
masked_score = -1000000000.0
F32 = jnp.float32
BF16 = jnp.bfloat16


def mm(a, b):
    return lax.dot_general(a, b, (((1,), (0,)), ((), ())), preferred_element_type=F32)


def mm_nt(a, b):
    return lax.dot_general(a, b, (((1,), (1,)), ((), ())), preferred_element_type=F32)


def mm_tn(a, b):
    return lax.dot_general(a, b, (((0,), (0,)), ((), ())), preferred_element_type=F32)


def group_of(n):
    return sum((n >= WLON * m).astype(jnp.int32) for m in range(1, PLACES))


def selection(lon_i):
    k = lax.broadcasted_iota(jnp.int32, (PLACES * OFFS, WIN), 0)
    n = lax.broadcasted_iota(jnp.int32, (1, WIN), 1)
    target = n + (OFFS - WLON) * group_of(n) + (WLON - 1) - lon_i
    return jnp.where(k == target, 1.0, 0.0).astype(BF16)


def core_kernel(
    air, up, east, north, corner, gain, w_qkv, w_proj, table,
    out24, out8, grads, d_table,
    x, y, xhat, rstd_s, normed, qkv, d_mix, bias, d_bias, acc_o, acc_dq, acc_dk, acc_dv, dqkv, mix, stage,
):
    lev, rows, cols, width = air.shape
    lev_wins, lon_wins = lev // WLEV, cols // WLON
    wins = lev_wins * lon_wins
    head_width = width // HEADS
    scale = head_width ** (-0.5)

    for src, (dst) in enumerate((x, y)):
        local = (air, up)[src]
        for rl in range(lev):
            a, l = divmod(rl, WLEV)
            ol = (rl + WLEV // 2) % lev
            for t in range(WLAT):
                p = l * WLAT + t
                if t < WLAT - LAT_SHIFT:
                    row = local[ol, t + LAT_SHIFT].astype(F32)
                    edge = east[src, ol, t + LAT_SHIFT].astype(F32)
                else:
                    row = north[src, ol, t - (WLAT - LAT_SHIFT)].astype(F32)
                    edge = corner[src, ol, t - (WLAT - LAT_SHIFT)].astype(F32)
                for c in range(lon_wins):
                    w = a * lon_wins + c
                    lo = LON_SHIFT + c * WLON
                    if c < lon_wins - 1:
                        dst[w, p * WLON:(p + 1) * WLON, :] = row[lo:lo + WLON]
                    else:
                        dst[w, p * WLON:p * WLON + WLON - LON_SHIFT, :] = row[lo:cols]
                        dst[w, p * WLON + WLON - LON_SHIFT:(p + 1) * WLON, :] = edge[:LON_SHIFT]

    t_val = table[...]
    t_hi = t_val.astype(BF16)
    t_rest = t_val - t_hi.astype(F32)
    t_mid = t_rest.astype(BF16)
    t_lo = (t_rest - t_mid.astype(F32)).astype(BF16)
    last_band = lax.axis_index("lat") == lax.axis_size("lat") - 1
    for lon_i in range(WLON):
        sel = selection(lon_i)
        b = mm(t_hi, sel) + mm(t_mid, sel) + mm(t_lo, sel)
        bias[:, lon_i, :] = b

    wq_all = w_qkv[...]
    for w in range(wins):
        xv = x[w]
        mean = jnp.mean(xv, axis=-1, keepdims=True)
        cen = xv - mean
        var = jnp.mean(cen * cen, axis=-1, keepdims=True)
        rs = lax.rsqrt(var + epsilon)
        xh = cen * rs
        xhat[w] = xh
        rstd_s[w] = rs
        nb = (xh * gain[...]).astype(BF16)
        normed[w] = nb
        res = mm(nb, wq_all).astype(BF16)
        for s in range(3):
            qkv[s, w] = res[:, s * width:(s + 1) * width]
        d_mix[w] = mm_nt(y[w].astype(BF16), w_proj[...]).astype(BF16)

    acc_o[...] = jnp.zeros_like(acc_o)
    acc_dq[...] = jnp.zeros_like(acc_dq)
    acc_dk[...] = jnp.zeros_like(acc_dk)
    acc_dv[...] = jnp.zeros_like(acc_dv)

    ri = lax.broadcasted_iota(jnp.int32, (WIN, WIN), 0)
    ci = lax.broadcasted_iota(jnp.int32, (WIN, WIN), 1)
    half = WIN // WLEV
    quarter = LAT_SHIFT * WLON

    def lev_of(n):
        return n >= half

    def lat_of(n):
        return jnp.where(n >= half, n - half, n) >= quarter

    lev_same = jnp.where(lev_of(ri) == lev_of(ci), 1, 0)
    lat_same = jnp.where(lat_of(ri) == lat_of(ci), 1, 0)
    lane = lax.broadcasted_iota(jnp.int32, (WIN, width), 1)

    def head_step(ah, carry):
        a = ah // HEADS
        h = ah - a * HEADS
        keep_lev = jnp.where(a == lev_wins - 1, 0, 1)
        keep_lat = jnp.where(last_band, 0, 1)
        same = ((lev_same + keep_lev) * (lat_same + keep_lat)) > 0
        bias_h = bias[pl.ds(ah * PLACES, PLACES)].reshape(WIN, WIN)
        bias_h = jnp.where(same, bias_h, masked_score)
        head = (lane >= h * head_width) & (lane < (h + 1) * head_width)
        d_bias_h = None
        for c in range(lon_wins):
            w = a * lon_wins + c
            q, k, v, dm = qkv[0, w], qkv[1, w], qkv[2, w], d_mix[w]
            zero = jnp.zeros_like(q)
            qm, km = jnp.where(head, q, zero), jnp.where(head, k, zero)
            vm, dmm = jnp.where(head, v, zero), jnp.where(head, dm, zero)
            s = mm_nt(q, km) * scale + bias_h
            m = jnp.max(s, axis=-1, keepdims=True)
            e = jnp.exp(s - m)
            pf = e / jnp.sum(e, axis=-1, keepdims=True)
            pb = pf.astype(BF16)
            acc_o[w] += mm(pb, vm)
            dp = mm_nt(dm, vm).astype(BF16).astype(F32)
            acc_dv[w] += mm_tn(pb, dmm)
            ds = pf * (dp - jnp.sum(dp * pf, axis=-1, keepdims=True))
            d_bias_h = ds if d_bias_h is None else d_bias_h + ds
            dsb = (ds * scale).astype(BF16)
            acc_dq[w] += mm(dsb, km)
            acc_dk[w] += mm_tn(dsb, qm)
        d_bias[pl.ds(ah * PLACES, PLACES)] = d_bias_h.reshape(PLACES, WLON, WIN)
        return carry

    lax.fori_loop(0, lev_wins * HEADS, head_step, 0)

    total = None
    for lon_i in range(WLON):
        part = mm_nt(d_bias[:, lon_i, :].astype(BF16), selection(lon_i))
        total = part if total is None else total + part
    t_parts, t_per, _ = d_table.shape
    for n in range(t_parts):
        d_table[n] = total[n * t_per:(n + 1) * t_per].astype(BF16)

    stage[...] = jnp.zeros_like(stage)
    d_gain = jnp.zeros((1, width), F32)
    for w in range(wins):
        a, c = divmod(w, lon_wins)
        mb = acc_o[w].astype(BF16)
        mix[w] = mb
        for s, acc in enumerate((acc_dq, acc_dk, acc_dv)):
            dqkv[w, :, s * width:(s + 1) * width] = acc[w].astype(BF16)
        branch = mm(mb, w_proj[...])
        d_pre = mm_nt(dqkv[w], wq_all)
        xh = xhat[w]
        d_gain = d_gain + jnp.sum(d_pre * xh, axis=0, keepdims=True)
        g = d_pre * gain[...]
        dx = rstd_s[w] * (
            g - jnp.mean(g, axis=-1, keepdims=True) - xh * jnp.mean(g * xh, axis=-1, keepdims=True)
        )
        for n, val in enumerate((branch, dx)):
            for p in range(PLACES):
                l, t = divmod(p, WLAT)
                ol = (a * WLEV + l + WLEV // 2) % lev
                lo = LON_SHIFT + c * WLON
                stage[n, ol, t, lo:lo + WLON, :] = val[p * WLON:(p + 1) * WLON]
    out24[...] = stage[:, :, :, 0:cols, :].astype(BF16)
    out8[...] = stage[:, :, :, cols:cols + EDGE, :].astype(BF16)

    dwq = None
    dwp = None
    for w in range(wins):
        one = mm_tn(normed[w], dqkv[w])
        two = mm_tn(mix[w], y[w].astype(BF16))
        dwq = one if dwq is None else dwq + one
        dwp = two if dwp is None else dwp + two
    parts, share, _ = grads.shape
    per = width // parts
    for n in range(parts):
        grads[n, 0:per, 0:3 * width] = dwq[n * per:(n + 1) * per].astype(BF16)
        grads[n, 0:per, 3 * width:4 * width] = dwp[n * per:(n + 1) * per].astype(BF16)
        grads[n, per:share, 0:width] = jnp.broadcast_to(d_gain, (share - per, width)).astype(BF16)
        grads[n, per:share, width:4 * width] = jnp.zeros((share - per, 3 * width), BF16)


def core_call(air, up, east, north, corner, gain, w_qkv, w_proj, table, parts):
    lev, rows, cols, width = air.shape
    wins = (lev // WLEV) * (cols // WLON)
    pairs = (lev // WLEV) * HEADS
    share = width // parts + 8
    vm = lambda shape, dtype: pltpu.VMEM(shape, dtype)
    win_f = vm((wins, WIN, width), F32)
    win_b = vm((wins, WIN, width), BF16)
    spec = pl.BlockSpec(memory_space=pltpu.VMEM)
    return pl.pallas_call(
        core_kernel,
        out_shape=(
            jax.ShapeDtypeStruct((2, lev, rows, cols, width), BF16),
            jax.ShapeDtypeStruct((2, lev, rows, EDGE, width), BF16),
            jax.ShapeDtypeStruct((parts, share, 4 * width), BF16),
            jax.ShapeDtypeStruct((parts, table.shape[0] // parts, table.shape[1]), BF16),
        ),
        in_specs=[spec] * 9,
        out_specs=(spec,) * 4,
        scratch_shapes=[
            win_f, win_f, win_f,
            vm((wins, WIN, 1), F32),
            win_b,
            vm((3, wins, WIN, width), BF16),
            win_b,
            vm((pairs * PLACES, WLON, WIN), F32),
            vm((pairs * PLACES, WLON, WIN), F32),
            win_f, win_f, win_f, win_f,
            vm((wins, WIN, 3 * width), BF16),
            win_b,
            vm((2, lev, rows, cols + EDGE, width), F32),
        ],
        compiler_params=pltpu.CompilerParams(vmem_limit_bytes=60 * 1024 * 1024),
        name="window_core",
    )(air, up, east, north, corner, gain, w_qkv, w_proj, table)


def spot(lon=0, lat=0):
    lon_at = lax.rem(lax.axis_index("lon") + lon + lax.axis_size("lon"), lax.axis_size("lon"))
    lat_at = lax.rem(lax.axis_index("lat") + lat + lax.axis_size("lat"), lax.axis_size("lat"))
    return {"lon": lon_at, "lat": lat_at}


def greet(places):
    barrier = pltpu.get_barrier_semaphore()
    for place in places:
        pl.semaphore_signal(barrier, inc=1, device_id=place, device_id_type=pl.DeviceIdType.MESH)
    pl.semaphore_wait(barrier, len(places))


def remote(src, dst, send, recv, place):
    return pltpu.make_async_remote_copy(
        src_ref=src, dst_ref=dst, send_sem=send, recv_sem=recv,
        device_id=place, device_id_type=pl.DeviceIdType.MESH,
    )


def halo_kernel(air, up, east, north, corner, send, recv):
    greet([spot(-1, 0), spot(0, -1), spot(-1, -1), spot(1, 0), spot(0, 1), spot(1, 1)])
    copies = []
    for n, src in enumerate((air, up)):
        rim = pl.ds(0, LAT_SHIFT)
        edge = pl.ds(0, EDGE)
        copies += [
            remote(src.at[:, rim], north.at[n], send.at[n, 0], recv.at[n, 0], spot(0, -1)),
            remote(src.at[:, :, edge], east.at[n], send.at[n, 1], recv.at[n, 1], spot(-1, 0)),
            remote(src.at[:, rim, edge], corner.at[n], send.at[n, 2], recv.at[n, 2], spot(-1, -1)),
        ]
    for copy in copies:
        copy.start()
    for copy in copies:
        copy.wait()


def halo_call(air, up):
    lev, rows, cols, width = air.shape
    spec = pl.BlockSpec(memory_space=pltpu.VMEM)
    return pl.pallas_call(
        halo_kernel,
        out_shape=(
            jax.ShapeDtypeStruct((2, lev, rows, EDGE, width), BF16),
            jax.ShapeDtypeStruct((2, lev, LAT_SHIFT, cols, width), BF16),
            jax.ShapeDtypeStruct((2, lev, LAT_SHIFT, EDGE, width), BF16),
        ),
        in_specs=[spec] * 2,
        out_specs=(spec,) * 3,
        scratch_shapes=[pltpu.SemaphoreType.DMA((2, 3)), pltpu.SemaphoreType.DMA((2, 3))],
        compiler_params=pltpu.CompilerParams(
            collective_id=0, has_side_effects=True, vmem_limit_bytes=40 * 1024 * 1024
        ),
        name="halo_in",
    )(air, up)


def finish_kernel(
    lons, lats, air, up, out24, out8, grads, table,
    block_out, d_state, d_gain, d_wqkv, d_wproj, d_table,
    got_n, got_e, got_c, land_w, land_t, land_lat, all_w, all_t,
    h_send, h_recv, w_send, w_recv, t_send, t_recv, l_send, l_recv, gw_send, gw_recv, gt_send, gt_recv,
):
    me, me_lat = lax.axis_index("lon"), lax.axis_index("lat")
    rows, width = air.shape[1], air.shape[3]
    keep = rows - LAT_SHIFT
    greet(
        [spot(k, 0) for k in range(1, lons)]
        + [spot(0, k) for k in range(1, lats)]
        + [spot(1, 1), spot(-1, -1)]
    )
    w_copies, t_copies = [], []
    for k in range(1, lons):
        to = spot(k, 0)
        w_copies.append(remote(grads.at[to["lon"]], land_w.at[k - 1], w_send.at[k - 1], w_recv.at[k - 1], to))
        t_copies.append(remote(table.at[to["lon"]], land_t.at[k - 1], t_send.at[k - 1], t_recv.at[k - 1], to))
    rim = pl.ds(keep, LAT_SHIFT)
    own = pl.ds(0, keep)
    halos = [
        remote(out24.at[:, :, rim], got_n, h_send.at[0], h_recv.at[0], spot(0, 1)),
        remote(out8.at[:, :, own], got_e, h_send.at[1], h_recv.at[1], spot(1, 0)),
        remote(out8.at[:, :, rim], got_c, h_send.at[2], h_recv.at[2], spot(1, 1)),
    ]
    for copy in w_copies + halos + t_copies:
        copy.start()

    total = grads[me].astype(F32)
    for k in range(1, lons):
        w_copies[k - 1].wait_recv()
        total = total + land_w[k - 1].astype(F32)
    land_lat[me_lat] = total.astype(BF16)
    l_copies = [
        remote(land_lat.at[me_lat], land_lat.at[me_lat], l_send.at[k - 1], l_recv.at[k - 1], spot(0, k))
        for k in range(1, lats)
    ]
    for copy in l_copies:
        copy.start()

    total = table[me].astype(F32)
    for k in range(1, lons):
        t_copies[k - 1].wait_recv()
        total = total + land_t[k - 1].astype(F32)
    all_t[me] = total.astype(BF16)
    gt_copies = [
        remote(all_t.at[me], all_t.at[me], gt_send.at[k - 1], gt_recv.at[k - 1], spot(k, 0))
        for k in range(1, lons)
    ]
    for copy in gt_copies:
        copy.start()

    for copy in halos:
        copy.wait_recv()
    for n, (src, dst) in enumerate(((air, block_out), (up, d_state))):
        for lv in range(air.shape[0]):
            for r in range(rows):
                base = src[lv, r].astype(F32)
                if r < LAT_SHIFT:
                    wide, edge = got_n[n, lv, r], got_c[n, lv, r]
                else:
                    wide, edge = out24[n, lv, r - LAT_SHIFT], got_e[n, lv, r - LAT_SHIFT]
                base = base + wide.astype(F32)
                head = base[:EDGE] + edge.astype(F32)
                dst[lv, r] = jnp.concatenate([head, base[EDGE:]], axis=0).astype(BF16)

    for copy in l_copies:
        copy.wait_recv()
    total = land_lat[0].astype(F32)
    for k in range(1, lats):
        total = total + land_lat[k].astype(F32)
    all_w[me] = total.astype(BF16)
    gw_copies = [
        remote(all_w.at[me], all_w.at[me], gw_send.at[k - 1], gw_recv.at[k - 1], spot(k, 0))
        for k in range(1, lons)
    ]
    for copy in gw_copies:
        copy.start()

    for copy in gt_copies:
        copy.wait_recv()
    d_table[...] = all_t[...].astype(F32)
    for copy in gw_copies:
        copy.wait_recv()
    per = width // lons
    d_wqkv[...] = all_w[:, 0:per, 0:3 * width].astype(F32)
    d_wproj[...] = all_w[:, 0:per, 3 * width:4 * width].astype(F32)
    d_gain[...] = all_w[0, per:per + 8, 0:width].astype(F32)
    for copy in w_copies + t_copies + halos + l_copies + gt_copies + gw_copies:
        copy.wait_send()


def finish_call(air, up, out24, out8, grads, table, lats):
    lev, rows, cols, width = air.shape
    lons, share, wide = grads.shape
    spec = pl.BlockSpec(memory_space=pltpu.VMEM)
    dma = pltpu.SemaphoreType.DMA
    per = width // lons
    return pl.pallas_call(
        partial(finish_kernel, lons, lats),
        out_shape=(
            jax.ShapeDtypeStruct(air.shape, BF16),
            jax.ShapeDtypeStruct(air.shape, BF16),
            jax.ShapeDtypeStruct((8, width), F32),
            jax.ShapeDtypeStruct((lons, per, 3 * width), F32),
            jax.ShapeDtypeStruct((lons, per, width), F32),
            jax.ShapeDtypeStruct(table.shape, F32),
        ),
        in_specs=[spec] * 6,
        out_specs=(spec,) * 6,
        scratch_shapes=[
            pltpu.VMEM((2, lev, LAT_SHIFT, cols, width), BF16),
            pltpu.VMEM((2, lev, rows - LAT_SHIFT, EDGE, width), BF16),
            pltpu.VMEM((2, lev, LAT_SHIFT, EDGE, width), BF16),
            pltpu.VMEM((lons - 1, share, wide), BF16),
            pltpu.VMEM((lons - 1,) + table.shape[1:], BF16),
            pltpu.VMEM((lats, share, wide), BF16),
            pltpu.VMEM(grads.shape, BF16),
            pltpu.VMEM(table.shape, BF16),
            dma((3,)), dma((3,)),
            dma((lons - 1,)), dma((lons - 1,)),
            dma((lons - 1,)), dma((lons - 1,)),
            dma((lats - 1,)), dma((lats - 1,)),
            dma((lons - 1,)), dma((lons - 1,)),
            dma((lons - 1,)), dma((lons - 1,)),
        ],
        compiler_params=pltpu.CompilerParams(
            collective_id=1, has_side_effects=True, vmem_limit_bytes=40 * 1024 * 1024
        ),
        name="finish",
    )(air, up, out24, out8, grads, table)


def on_device(air_state, upstream, norm_gain, w_qkv, w_proj, bias_table):
    lev, rows, cols, width = air_state.shape
    lons, lats = lax.axis_size("lon"), lax.axis_size("lat")
    pairs = (lev // WLEV) * HEADS
    east, north, corner = halo_call(air_state, upstream)
    out24, out8, grads, d_table = core_call(
        air_state, upstream, east, north, corner, norm_gain.reshape(1, width), w_qkv, w_proj,
        bias_table.reshape(pairs * PLACES, PLACES * OFFS), lons,
    )
    block_out, d_state, d_gain, d_wqkv, d_wproj, d_table = finish_call(
        air_state, upstream, out24, out8, grads, d_table, lats
    )
    return (
        block_out, d_state, d_gain[0], d_wqkv.reshape(width, 3 * width), d_wproj.reshape(width, width),
        d_table.reshape(bias_table.shape),
    )


def solution(mesh):
    return jax.shard_map(
        on_device,
        mesh=mesh,
        in_specs=(
            P(None, "lat", "lon", None),
            P(None, "lat", "lon", None),
            P(),
            P(),
            P(),
            P("lat", None, None, None),
        ),
        out_specs=(
            P(None, "lat", "lon", None),
            P(None, "lat", "lon", None),
            P(),
            P(),
            P(),
            P("lat", None, None, None),
        ),
        check_vma=False,
    )
```

```python
from functools import partial

import jax
import jax.numpy as jnp
from jax import lax
from jax.experimental import pallas as pl
from jax.experimental.pallas import tpu as pltpu
from jax.sharding import PartitionSpec as P

HEADS = 6
WLEV = 2
WLAT = 6
WLON = 12
WIN = 144
PLACES = WLEV * WLAT
OFFS = 2 * WLON - 1
LAT_SHIFT = WLAT // 2
LON_SHIFT = WLON // 2
EDGE = 8

epsilon = 1e-05
masked_score = -1000000000.0
F32 = jnp.float32
BF16 = jnp.bfloat16


def mm(a, b):
    return lax.dot_general(a, b, (((1,), (0,)), ((), ())), preferred_element_type=F32)


def mm_nt(a, b):
    return lax.dot_general(a, b, (((1,), (1,)), ((), ())), preferred_element_type=F32)


def mm_tn(a, b):
    return lax.dot_general(a, b, (((0,), (0,)), ((), ())), preferred_element_type=F32)


def group_of(n):
    return sum((n >= WLON * m).astype(jnp.int32) for m in range(1, PLACES))


def selection(lon_i):
    k = lax.broadcasted_iota(jnp.int32, (PLACES * OFFS, WIN), 0)
    n = lax.broadcasted_iota(jnp.int32, (1, WIN), 1)
    target = n + (OFFS - WLON) * group_of(n) + (WLON - 1) - lon_i
    return jnp.where(k == target, 1.0, 0.0).astype(BF16)


def core_kernel(
    air, up, east, north, corner, gain, w_qkv, w_proj, table,
    out24, out8, grads, d_table,
    x, y, xhat, rstd_s, normed, qkv, d_mix, bias, d_bias, acc_o, acc_dq, acc_dk, acc_dv, dqkv, mix, stage,
):
    lev, rows, cols, width = air.shape
    lev_wins, lon_wins = lev // WLEV, cols // WLON
    wins = lev_wins * lon_wins
    head_width = width // HEADS
    scale = head_width ** (-0.5)

    for src, (dst) in enumerate((x, y)):
        local = (air, up)[src]
        for rl in range(lev):
            a, l = divmod(rl, WLEV)
            ol = (rl + WLEV // 2) % lev
            for t in range(WLAT):
                p = l * WLAT + t
                if t < WLAT - LAT_SHIFT:
                    row = local[ol, t + LAT_SHIFT].astype(F32)
                    edge = east[src, ol, t + LAT_SHIFT].astype(F32)
                else:
                    row = north[src, ol, t - (WLAT - LAT_SHIFT)].astype(F32)
                    edge = corner[src, ol, t - (WLAT - LAT_SHIFT)].astype(F32)
                for c in range(lon_wins):
                    w = a * lon_wins + c
                    lo = LON_SHIFT + c * WLON
                    if c < lon_wins - 1:
                        dst[w, p * WLON:(p + 1) * WLON, :] = row[lo:lo + WLON]
                    else:
                        dst[w, p * WLON:p * WLON + WLON - LON_SHIFT, :] = row[lo:cols]
                        dst[w, p * WLON + WLON - LON_SHIFT:(p + 1) * WLON, :] = edge[:LON_SHIFT]

    t_val = table[...]
    t_hi = t_val.astype(BF16)
    t_rest = t_val - t_hi.astype(F32)
    t_mid = t_rest.astype(BF16)
    t_lo = (t_rest - t_mid.astype(F32)).astype(BF16)
    last_band = lax.axis_index("lat") == lax.axis_size("lat") - 1
    for lon_i in range(WLON):
        sel = selection(lon_i)
        b = mm(t_hi, sel) + mm(t_mid, sel) + mm(t_lo, sel)
        bias[:, lon_i, :] = b

    wq_all = w_qkv[...]
    for w in range(wins):
        xv = x[w]
        mean = jnp.mean(xv, axis=-1, keepdims=True)
        cen = xv - mean
        var = jnp.mean(cen * cen, axis=-1, keepdims=True)
        rs = lax.rsqrt(var + epsilon)
        xh = cen * rs
        xhat[w] = xh
        rstd_s[w] = rs
        nb = (xh * gain[...]).astype(BF16)
        normed[w] = nb
        res = mm(nb, wq_all).astype(BF16)
        for s in range(3):
            qkv[s, w] = res[:, s * width:(s + 1) * width]
        d_mix[w] = mm_nt(y[w].astype(BF16), w_proj[...]).astype(BF16)

    acc_o[...] = jnp.zeros_like(acc_o)
    acc_dq[...] = jnp.zeros_like(acc_dq)
    acc_dk[...] = jnp.zeros_like(acc_dk)
    acc_dv[...] = jnp.zeros_like(acc_dv)

    ri = lax.broadcasted_iota(jnp.int32, (WIN, WIN), 0)
    ci = lax.broadcasted_iota(jnp.int32, (WIN, WIN), 1)
    half = WIN // WLEV
    quarter = LAT_SHIFT * WLON

    def lev_of(n):
        return n >= half

    def lat_of(n):
        return jnp.where(n >= half, n - half, n) >= quarter

    lev_same = jnp.where(lev_of(ri) == lev_of(ci), 1, 0)
    lat_same = jnp.where(lat_of(ri) == lat_of(ci), 1, 0)
    lane = lax.broadcasted_iota(jnp.int32, (WIN, width), 1)

    def head_step(ah, carry):
        a = ah // HEADS
        h = ah - a * HEADS
        keep_lev = jnp.where(a == lev_wins - 1, 0, 1)
        keep_lat = jnp.where(last_band, 0, 1)
        same = ((lev_same + keep_lev) * (lat_same + keep_lat)) > 0
        bias_h = bias[pl.ds(ah * PLACES, PLACES)].reshape(WIN, WIN)
        bias_h = jnp.where(same, bias_h, masked_score)
        head = (lane >= h * head_width) & (lane < (h + 1) * head_width)
        d_bias_h = None
        for c in range(lon_wins):
            w = a * lon_wins + c
            q, k, v, dm = qkv[0, w], qkv[1, w], qkv[2, w], d_mix[w]
            zero = jnp.zeros_like(q)
            qm, km = jnp.where(head, q, zero), jnp.where(head, k, zero)
            vm, dmm = jnp.where(head, v, zero), jnp.where(head, dm, zero)
            s = mm_nt(q, km) * scale + bias_h
            m = jnp.max(s, axis=-1, keepdims=True)
            e = jnp.exp(s - m)
            pf = e / jnp.sum(e, axis=-1, keepdims=True)
            pb = pf.astype(BF16)
            acc_o[w] += mm(pb, vm)
            dp = mm_nt(dm, vm).astype(BF16).astype(F32)
            acc_dv[w] += mm_tn(pb, dmm)
            ds = pf * (dp - jnp.sum(dp * pf, axis=-1, keepdims=True))
            d_bias_h = ds if d_bias_h is None else d_bias_h + ds
            dsb = (ds * scale).astype(BF16)
            acc_dq[w] += mm(dsb, km)
            acc_dk[w] += mm_tn(dsb, qm)
        d_bias[pl.ds(ah * PLACES, PLACES)] = d_bias_h.reshape(PLACES, WLON, WIN)
        return carry

    lax.fori_loop(0, lev_wins * HEADS, head_step, 0, unroll=2)

    total = None
    for lon_i in range(WLON):
        part = mm_nt(d_bias[:, lon_i, :].astype(BF16), selection(lon_i))
        total = part if total is None else total + part
    t_total = total

    stage[...] = jnp.zeros_like(stage)
    d_gain = jnp.zeros((1, width), F32)
    for w in range(wins):
        a, c = divmod(w, lon_wins)
        mb = acc_o[w].astype(BF16)
        mix[w] = mb
        for s, acc in enumerate((acc_dq, acc_dk, acc_dv)):
            dqkv[w, :, s * width:(s + 1) * width] = acc[w].astype(BF16)
        branch = mm(mb, w_proj[...])
        d_pre = mm_nt(dqkv[w], wq_all)
        xh = xhat[w]
        d_gain = d_gain + jnp.sum(d_pre * xh, axis=0, keepdims=True)
        g = d_pre * gain[...]
        dx = rstd_s[w] * (
            g - jnp.mean(g, axis=-1, keepdims=True) - xh * jnp.mean(g * xh, axis=-1, keepdims=True)
        )
        for n, val in enumerate((branch, dx)):
            for p in range(PLACES):
                l, t = divmod(p, WLAT)
                ol = (a * WLEV + l + WLEV // 2) % lev
                lo = LON_SHIFT + c * WLON
                stage[n, ol, t, lo:lo + WLON, :] = val[p * WLON:(p + 1) * WLON]
    out24[...] = stage[:, :, :, 0:cols, :].astype(BF16)
    out8[...] = stage[:, :, :, cols:cols + EDGE, :].astype(BF16)

    dwq = None
    dwp = None
    for w in range(wins):
        one = mm_tn(normed[w], dqkv[w])
        two = mm_tn(mix[w], y[w].astype(BF16))
        dwq = one if dwq is None else dwq + one
        dwp = two if dwp is None else dwp + two
    parts, per, _ = grads.shape
    t_share = d_table.shape[1]
    t_per = t_total.shape[0] // parts
    filler = jnp.concatenate([d_gain, jnp.zeros((1, t_total.shape[1] - width), F32)], axis=1)
    filler = jnp.broadcast_to(filler, (t_share - t_per, t_total.shape[1]))
    for n in range(parts):
        grads[n, :, 0:3 * width] = dwq[n * per:(n + 1) * per].astype(BF16)
        grads[n, :, 3 * width:4 * width] = dwp[n * per:(n + 1) * per].astype(BF16)
        rows_n = jnp.concatenate([t_total[n * t_per:(n + 1) * t_per], filler], axis=0)
        d_table[n] = rows_n.astype(BF16)


def core_call(air, up, east, north, corner, gain, w_qkv, w_proj, table, parts):
    lev, rows, cols, width = air.shape
    wins = (lev // WLEV) * (cols // WLON)
    pairs = (lev // WLEV) * HEADS
    t_share = table.shape[0] // parts // 8 * 8 + 8
    vm = lambda shape, dtype: pltpu.VMEM(shape, dtype)
    win_f = vm((wins, WIN, width), F32)
    win_b = vm((wins, WIN, width), BF16)
    spec = pl.BlockSpec(memory_space=pltpu.VMEM)
    return pl.pallas_call(
        core_kernel,
        out_shape=(
            jax.ShapeDtypeStruct((2, lev, rows, cols, width), BF16),
            jax.ShapeDtypeStruct((2, lev, rows, EDGE, width), BF16),
            jax.ShapeDtypeStruct((parts, width // parts, 4 * width), BF16),
            jax.ShapeDtypeStruct((parts, t_share, table.shape[1]), BF16),
        ),
        in_specs=[spec] * 9,
        out_specs=(spec,) * 4,
        scratch_shapes=[
            win_f, win_f, win_f,
            vm((wins, WIN, 1), F32),
            win_b,
            vm((3, wins, WIN, width), BF16),
            win_b,
            vm((pairs * PLACES, WLON, WIN), F32),
            vm((pairs * PLACES, WLON, WIN), F32),
            win_f, win_f, win_f, win_f,
            vm((wins, WIN, 3 * width), BF16),
            win_b,
            vm((2, lev, rows, cols + EDGE, width), F32),
        ],
        compiler_params=pltpu.CompilerParams(vmem_limit_bytes=26 * 1024 * 1024),
        name="window_core",
    )(air, up, east, north, corner, gain, w_qkv, w_proj, table)


def spot(lon=0, lat=0):
    lon_at = lax.rem(lax.axis_index("lon") + lon + lax.axis_size("lon"), lax.axis_size("lon"))
    lat_at = lax.rem(lax.axis_index("lat") + lat + lax.axis_size("lat"), lax.axis_size("lat"))
    return {"lon": lon_at, "lat": lat_at}


def greet(places):
    barrier = pltpu.get_barrier_semaphore()
    for place in places:
        pl.semaphore_signal(barrier, inc=1, device_id=place, device_id_type=pl.DeviceIdType.MESH)
    pl.semaphore_wait(barrier, len(places))


def remote(src, dst, send, recv, place):
    return pltpu.make_async_remote_copy(
        src_ref=src, dst_ref=dst, send_sem=send, recv_sem=recv,
        device_id=place, device_id_type=pl.DeviceIdType.MESH,
    )


def halo_kernel(air, up, east, north, corner, send, recv):
    greet([spot(-1, 0), spot(0, -1), spot(-1, -1), spot(1, 0), spot(0, 1), spot(1, 1)])
    copies = []
    for n, src in enumerate((air, up)):
        rim = pl.ds(0, LAT_SHIFT)
        edge = pl.ds(0, EDGE)
        copies += [
            remote(src.at[:, rim], north.at[n], send.at[n, 0], recv.at[n, 0], spot(0, -1)),
            remote(src.at[:, :, edge], east.at[n], send.at[n, 1], recv.at[n, 1], spot(-1, 0)),
            remote(src.at[:, rim, edge], corner.at[n], send.at[n, 2], recv.at[n, 2], spot(-1, -1)),
        ]
    for copy in copies:
        copy.start()
    for copy in copies:
        copy.wait()


def halo_call(air, up):
    lev, rows, cols, width = air.shape
    spec = pl.BlockSpec(memory_space=pltpu.VMEM)
    return pl.pallas_call(
        halo_kernel,
        out_shape=(
            jax.ShapeDtypeStruct((2, lev, rows, EDGE, width), BF16),
            jax.ShapeDtypeStruct((2, lev, LAT_SHIFT, cols, width), BF16),
            jax.ShapeDtypeStruct((2, lev, LAT_SHIFT, EDGE, width), BF16),
        ),
        in_specs=[spec] * 2,
        out_specs=(spec,) * 3,
        scratch_shapes=[pltpu.SemaphoreType.DMA((2, 3)), pltpu.SemaphoreType.DMA((2, 3))],
        compiler_params=pltpu.CompilerParams(
            collective_id=0, has_side_effects=True, vmem_limit_bytes=8 * 1024 * 1024
        ),
        name="halo_in",
    )(air, up)


def finish_kernel(
    lons, lats, air, up, out24, out8, grads, table,
    block_out, d_state, d_gain, d_wqkv, d_wproj, d_table,
    got_n, got_e, got_c, land_w, land_t, land_lat, all_w, all_t, land_g,
    h_send, h_recv, w_send, w_recv, t_send, t_recv, l_send, l_recv, gw_send, gw_recv, gt_send, gt_recv, g_send, g_recv,
):
    me, me_lat = lax.axis_index("lon"), lax.axis_index("lat")
    rows, width = air.shape[1], air.shape[3]
    keep = rows - LAT_SHIFT
    greet(
        [spot(k, 0) for k in range(1, lons)]
        + [spot(0, k) for k in range(1, lats)]
        + [spot(1, 1), spot(-1, -1)]
    )
    w_copies, t_copies = [], []
    for k in range(1, lons):
        to = spot(k, 0)
        w_copies.append(remote(grads.at[to["lon"]], land_w.at[k - 1], w_send.at[k - 1], w_recv.at[k - 1], to))
        t_copies.append(remote(table.at[to["lon"]], land_t.at[me], t_send.at[k - 1], t_recv.at[k - 1], to))
    rim = pl.ds(keep, LAT_SHIFT)
    own = pl.ds(0, keep)
    halos = [
        remote(out24.at[:, :, rim], got_n, h_send.at[0], h_recv.at[0], spot(0, 1)),
        remote(out8.at[:, :, own], got_e, h_send.at[1], h_recv.at[1], spot(1, 0)),
        remote(out8.at[:, :, rim], got_c, h_send.at[2], h_recv.at[2], spot(1, 1)),
    ]
    for copy in w_copies + halos + t_copies:
        copy.start()

    total = grads[me].astype(F32)
    for k in range(1, lons):
        w_copies[k - 1].wait_recv()
        total = total + land_w[k - 1].astype(F32)
    land_lat[me_lat] = total.astype(BF16)
    l_copies = [
        remote(land_lat.at[me_lat], land_lat.at[me_lat], l_send.at[k - 1], l_recv.at[k - 1], spot(0, k))
        for k in range(1, lats)
    ]
    for copy in l_copies:
        copy.start()

    land_t[me] = table[me]
    for k in range(1, lons):
        t_copies[k - 1].wait_recv()
    total = land_t[0].astype(F32)
    for n in range(1, lons):
        total = total + land_t[n].astype(F32)
    t_share = table.shape[1]
    land_g[me_lat] = total[t_share - 8:].astype(BF16)
    g_copies = [
        remote(land_g.at[me_lat], land_g.at[me_lat], g_send.at[k - 1], g_recv.at[k - 1], spot(0, k))
        for k in range(1, lats)
    ]
    for copy in g_copies:
        copy.start()
    all_t[me] = total.astype(BF16)
    gt_copies = [
        remote(all_t.at[me], all_t.at[me], gt_send.at[k - 1], gt_recv.at[k - 1], spot(k, 0))
        for k in range(1, lons)
    ]
    for copy in gt_copies:
        copy.start()

    for copy in halos:
        copy.wait_recv()
    for n, (src, dst) in enumerate(((air, block_out), (up, d_state))):
        for lv in range(air.shape[0]):
            for r in range(rows):
                base = src[lv, r].astype(F32)
                if r < LAT_SHIFT:
                    wide, edge = got_n[n, lv, r], got_c[n, lv, r]
                else:
                    wide, edge = out24[n, lv, r - LAT_SHIFT], got_e[n, lv, r - LAT_SHIFT]
                base = base + wide.astype(F32)
                head = base[:EDGE] + edge.astype(F32)
                dst[lv, r] = jnp.concatenate([head, base[EDGE:]], axis=0).astype(BF16)

    for copy in l_copies:
        copy.wait_recv()
    total = land_lat[0].astype(F32)
    for k in range(1, lats):
        total = total + land_lat[k].astype(F32)
    all_w[me] = total.astype(BF16)
    gw_copies = [
        remote(all_w.at[me], all_w.at[me], gw_send.at[k - 1], gw_recv.at[k - 1], spot(k, 0))
        for k in range(1, lons)
    ]
    for copy in gw_copies:
        copy.start()

    for copy in g_copies:
        copy.wait_recv()
    total = land_g[0].astype(F32)
    for k in range(1, lats):
        total = total + land_g[k].astype(F32)
    d_gain[...] = total[:, 0:width]
    for copy in gt_copies:
        copy.wait_recv()
    d_table[...] = all_t[:, 0:d_table.shape[1]].astype(F32)
    for copy in gw_copies:
        copy.wait_recv()
    d_wqkv[...] = all_w[:, :, 0:3 * width].astype(F32)
    d_wproj[...] = all_w[:, :, 3 * width:4 * width].astype(F32)
    for copy in w_copies + t_copies + halos + l_copies + gt_copies + gw_copies + g_copies:
        copy.wait_send()


def finish_call(air, up, out24, out8, grads, table, lats, t_per):
    lev, rows, cols, width = air.shape
    lons, share, wide = grads.shape
    spec = pl.BlockSpec(memory_space=pltpu.VMEM)
    dma = pltpu.SemaphoreType.DMA
    per = width // lons
    return pl.pallas_call(
        partial(finish_kernel, lons, lats),
        out_shape=(
            jax.ShapeDtypeStruct(air.shape, BF16),
            jax.ShapeDtypeStruct(air.shape, BF16),
            jax.ShapeDtypeStruct((8, width), F32),
            jax.ShapeDtypeStruct((lons, per, 3 * width), F32),
            jax.ShapeDtypeStruct((lons, per, width), F32),
            jax.ShapeDtypeStruct((lons, t_per, table.shape[2]), F32),
        ),
        in_specs=[spec] * 6,
        out_specs=(spec,) * 6,
        scratch_shapes=[
            pltpu.VMEM((2, lev, LAT_SHIFT, cols, width), BF16),
            pltpu.VMEM((2, lev, rows - LAT_SHIFT, EDGE, width), BF16),
            pltpu.VMEM((2, lev, LAT_SHIFT, EDGE, width), BF16),
            pltpu.VMEM((lons - 1, share, wide), BF16),
            pltpu.VMEM(table.shape, BF16),
            pltpu.VMEM((lats, share, wide), BF16),
            pltpu.VMEM(grads.shape, BF16),
            pltpu.VMEM(table.shape, BF16),
            pltpu.VMEM((lats, 8, table.shape[2]), BF16),
            dma((3,)), dma((3,)),
            dma((lons - 1,)), dma((lons - 1,)),
            dma((lons - 1,)), dma((lons - 1,)),
            dma((lats - 1,)), dma((lats - 1,)),
            dma((lons - 1,)), dma((lons - 1,)),
            dma((lons - 1,)), dma((lons - 1,)),
            dma((lats - 1,)), dma((lats - 1,)),
        ],
        compiler_params=pltpu.CompilerParams(
            collective_id=1, has_side_effects=True, vmem_limit_bytes=20 * 1024 * 1024
        ),
        name="finish",
    )(air, up, out24, out8, grads, table)


def on_device(air_state, upstream, norm_gain, w_qkv, w_proj, bias_table):
    lev, rows, cols, width = air_state.shape
    lons, lats = lax.axis_size("lon"), lax.axis_size("lat")
    pairs = (lev // WLEV) * HEADS
    east, north, corner = halo_call(air_state, upstream)
    out24, out8, grads, d_table = core_call(
        air_state, upstream, east, north, corner, norm_gain.reshape(1, width), w_qkv, w_proj,
        bias_table.reshape(pairs * PLACES, PLACES * OFFS), lons,
    )
    block_out, d_state, d_gain, d_wqkv, d_wproj, d_table = finish_call(
        air_state, upstream, out24, out8, grads, d_table, lats, pairs * PLACES // lons
    )
    return (
        block_out, d_state, d_gain[7], d_wqkv.reshape(width, 3 * width), d_wproj.reshape(width, width),
        d_table.reshape(bias_table.shape),
    )


def solution(mesh):
    return jax.shard_map(
        on_device,
        mesh=mesh,
        in_specs=(
            P(None, "lat", "lon", None),
            P(None, "lat", "lon", None),
            P(),
            P(),
            P(),
            P("lat", None, None, None),
        ),
        out_specs=(
            P(None, "lat", "lon", None),
            P(None, "lat", "lon", None),
            P(),
            P(),
            P(),
            P("lat", None, None, None),
        ),
        check_vma=False,
    )
```

```python
from functools import partial

import jax
import jax.numpy as jnp
from jax import lax
from jax.experimental import pallas as pl
from jax.experimental.pallas import tpu as pltpu
from jax.sharding import PartitionSpec as P

HEADS = 6
WLEV = 2
WLAT = 6
WLON = 12
WIN = 144
PLACES = WLEV * WLAT
OFFS = 2 * WLON - 1
LAT_SHIFT = WLAT // 2
LON_SHIFT = WLON // 2
EDGE = 8

epsilon = 1e-05
masked_score = -1000000000.0
F32 = jnp.float32
BF16 = jnp.bfloat16


def mm(a, b):
    return lax.dot_general(a, b, (((1,), (0,)), ((), ())), preferred_element_type=F32)


def mm_nt(a, b):
    return lax.dot_general(a, b, (((1,), (1,)), ((), ())), preferred_element_type=F32)


def mm_tn(a, b):
    return lax.dot_general(a, b, (((0,), (0,)), ((), ())), preferred_element_type=F32)


def group_of(n):
    return sum((n >= WLON * m).astype(jnp.int32) for m in range(1, PLACES))


def selection(lon_i):
    k = lax.broadcasted_iota(jnp.int32, (PLACES * OFFS, WIN), 0)
    n = lax.broadcasted_iota(jnp.int32, (1, WIN), 1)
    target = n + (OFFS - WLON) * group_of(n) + (WLON - 1) - lon_i
    return jnp.where(k == target, 1.0, 0.0).astype(BF16)


def core_kernel(
    air, up, east, north, corner, gain, w_qkv, w_proj, bias,
    out24, out8, grads, d_table,
    x, y, xhat, rstd_s, normed, qkv, d_mix, d_bias, acc_o, acc_dq, acc_dk, acc_dv, dqkv, mix, stage,
):
    lev, rows, cols, width = air.shape
    lev_wins, lon_wins = lev // WLEV, cols // WLON
    wins = lev_wins * lon_wins
    head_width = width // HEADS
    scale = head_width ** (-0.5)

    for src, (dst) in enumerate((x, y)):
        local = (air, up)[src]
        for rl in range(lev):
            a, l = divmod(rl, WLEV)
            ol = (rl + WLEV // 2) % lev
            for t in range(WLAT):
                p = l * WLAT + t
                if t < WLAT - LAT_SHIFT:
                    row = local[ol, t + LAT_SHIFT].astype(F32)
                    edge = east[src, ol, t + LAT_SHIFT].astype(F32)
                else:
                    row = north[src, ol, t - (WLAT - LAT_SHIFT)].astype(F32)
                    edge = corner[src, ol, t - (WLAT - LAT_SHIFT)].astype(F32)
                for c in range(lon_wins):
                    w = a * lon_wins + c
                    lo = LON_SHIFT + c * WLON
                    if c < lon_wins - 1:
                        dst[w, p * WLON:(p + 1) * WLON, :] = row[lo:lo + WLON]
                    else:
                        dst[w, p * WLON:p * WLON + WLON - LON_SHIFT, :] = row[lo:cols]
                        dst[w, p * WLON + WLON - LON_SHIFT:(p + 1) * WLON, :] = edge[:LON_SHIFT]

    last_band = lax.axis_index("lat") == lax.axis_size("lat") - 1
    wq_all = w_qkv[...]
    for w in range(wins):
        xv = x[w]
        mean = jnp.mean(xv, axis=-1, keepdims=True)
        cen = xv - mean
        var = jnp.mean(cen * cen, axis=-1, keepdims=True)
        rs = lax.rsqrt(var + epsilon)
        xh = cen * rs
        xhat[w] = xh
        rstd_s[w] = rs
        nb = (xh * gain[...]).astype(BF16)
        normed[w] = nb
        res = mm(nb, wq_all).astype(BF16)
        for s in range(3):
            qkv[s, w] = res[:, s * width:(s + 1) * width]
        d_mix[w] = mm_nt(y[w].astype(BF16), w_proj[...]).astype(BF16)

    acc_o[...] = jnp.zeros_like(acc_o)
    acc_dq[...] = jnp.zeros_like(acc_dq)
    acc_dk[...] = jnp.zeros_like(acc_dk)
    acc_dv[...] = jnp.zeros_like(acc_dv)

    ri = lax.broadcasted_iota(jnp.int32, (WIN, WIN), 0)
    ci = lax.broadcasted_iota(jnp.int32, (WIN, WIN), 1)
    half = WIN // WLEV
    quarter = LAT_SHIFT * WLON

    def lev_of(n):
        return n >= half

    def lat_of(n):
        return jnp.where(n >= half, n - half, n) >= quarter

    lev_same = jnp.where(lev_of(ri) == lev_of(ci), 1, 0)
    lat_same = jnp.where(lat_of(ri) == lat_of(ci), 1, 0)
    lane = lax.broadcasted_iota(jnp.int32, (WIN, width), 1)

    def head_step(ah, carry):
        a = ah // HEADS
        h = ah - a * HEADS
        keep_lev = jnp.where(a == lev_wins - 1, 0, 1)
        keep_lat = jnp.where(last_band, 0, 1)
        same = ((lev_same + keep_lev) * (lat_same + keep_lat)) > 0
        bias_h = bias[pl.ds(ah * PLACES, PLACES)].reshape(WIN, WIN)
        bias_h = jnp.where(same, bias_h, masked_score)
        head = (lane >= h * head_width) & (lane < (h + 1) * head_width)
        d_bias_h = None
        for c in range(lon_wins):
            w = a * lon_wins + c
            q, k, v, dm = qkv[0, w], qkv[1, w], qkv[2, w], d_mix[w]
            zero = jnp.zeros_like(q)
            qm, km = jnp.where(head, q, zero), jnp.where(head, k, zero)
            vm, dmm = jnp.where(head, v, zero), jnp.where(head, dm, zero)
            s = mm_nt(q, km) * scale + bias_h
            m = jnp.max(s, axis=-1, keepdims=True)
            e = jnp.exp(s - m)
            pf = e / jnp.sum(e, axis=-1, keepdims=True)
            pb = pf.astype(BF16)
            acc_o[w] += mm(pb, vm)
            dp = mm_nt(dm, vm).astype(BF16).astype(F32)
            acc_dv[w] += mm_tn(pb, dmm)
            ds = pf * (dp - jnp.sum(dp * pf, axis=-1, keepdims=True))
            d_bias_h = ds if d_bias_h is None else d_bias_h + ds
            dsb = (ds * scale).astype(BF16)
            acc_dq[w] += mm(dsb, km)
            acc_dk[w] += mm_tn(dsb, qm)
        d_bias[pl.ds(ah * PLACES, PLACES)] = d_bias_h.reshape(PLACES, WLON, WIN)
        return carry

    lax.fori_loop(0, lev_wins * HEADS, head_step, 0, unroll=4)

    total = None
    for lon_i in range(WLON):
        part = mm_nt(d_bias[:, lon_i, :].astype(BF16), selection(lon_i))
        total = part if total is None else total + part
    t_total = total

    stage[...] = jnp.zeros_like(stage)
    d_gain = jnp.zeros((1, width), F32)
    for w in range(wins):
        a, c = divmod(w, lon_wins)
        mb = acc_o[w].astype(BF16)
        mix[w] = mb
        for s, acc in enumerate((acc_dq, acc_dk, acc_dv)):
            dqkv[w, :, s * width:(s + 1) * width] = acc[w].astype(BF16)
        branch = mm(mb, w_proj[...])
        d_pre = mm_nt(dqkv[w], wq_all)
        xh = xhat[w]
        d_gain = d_gain + jnp.sum(d_pre * xh, axis=0, keepdims=True)
        g = d_pre * gain[...]
        dx = rstd_s[w] * (
            g - jnp.mean(g, axis=-1, keepdims=True) - xh * jnp.mean(g * xh, axis=-1, keepdims=True)
        )
        for n, val in enumerate((branch, dx)):
            for p in range(PLACES):
                l, t = divmod(p, WLAT)
                ol = (a * WLEV + l + WLEV // 2) % lev
                lo = LON_SHIFT + c * WLON
                stage[n, ol, t, lo:lo + WLON, :] = val[p * WLON:(p + 1) * WLON]
    out24[...] = stage[:, :, :, 0:cols, :].astype(BF16)
    out8[...] = stage[:, :, :, cols:cols + EDGE, :].astype(BF16)

    dwq = None
    dwp = None
    for w in range(wins):
        one = mm_tn(normed[w], dqkv[w])
        two = mm_tn(mix[w], y[w].astype(BF16))
        dwq = one if dwq is None else dwq + one
        dwp = two if dwp is None else dwp + two
    parts, per, _ = grads.shape
    t_share = d_table.shape[1]
    t_per = t_total.shape[0] // parts
    filler = jnp.concatenate([d_gain, jnp.zeros((1, t_total.shape[1] - width), F32)], axis=1)
    filler = jnp.broadcast_to(filler, (t_share - t_per, t_total.shape[1]))
    for n in range(parts):
        grads[n, :, 0:3 * width] = dwq[n * per:(n + 1) * per].astype(BF16)
        grads[n, :, 3 * width:4 * width] = dwp[n * per:(n + 1) * per].astype(BF16)
        rows_n = jnp.concatenate([t_total[n * t_per:(n + 1) * t_per], filler], axis=0)
        d_table[n] = rows_n.astype(BF16)


def core_call(air, up, east, north, corner, gain, w_qkv, w_proj, bias, parts):
    lev, rows, cols, width = air.shape
    wins = (lev // WLEV) * (cols // WLON)
    pairs = (lev // WLEV) * HEADS
    t_share = pairs * PLACES // parts // 8 * 8 + 8
    vm = lambda shape, dtype: pltpu.VMEM(shape, dtype)
    win_f = vm((wins, WIN, width), F32)
    win_b = vm((wins, WIN, width), BF16)
    spec = pl.BlockSpec(memory_space=pltpu.VMEM)
    return pl.pallas_call(
        core_kernel,
        out_shape=(
            jax.ShapeDtypeStruct((2, lev, rows, cols, width), BF16),
            jax.ShapeDtypeStruct((2, lev, rows, EDGE, width), BF16),
            jax.ShapeDtypeStruct((parts, width // parts, 4 * width), BF16),
            jax.ShapeDtypeStruct((parts, t_share, PLACES * OFFS), BF16),
        ),
        in_specs=[spec] * 9,
        out_specs=(spec,) * 4,
        scratch_shapes=[
            win_f, win_f, win_f,
            vm((wins, WIN, 1), F32),
            win_b,
            vm((3, wins, WIN, width), BF16),
            win_b,
            vm((pairs * PLACES, WLON, WIN), F32),
            win_f, win_f, win_f, win_f,
            vm((wins, WIN, 3 * width), BF16),
            win_b,
            vm((2, lev, rows, cols + EDGE, width), F32),
        ],
        compiler_params=pltpu.CompilerParams(vmem_limit_bytes=26 * 1024 * 1024),
        name="window_core",
    )(air, up, east, north, corner, gain, w_qkv, w_proj, bias)


def spot(lon=0, lat=0):
    lon_at = lax.rem(lax.axis_index("lon") + lon + lax.axis_size("lon"), lax.axis_size("lon"))
    lat_at = lax.rem(lax.axis_index("lat") + lat + lax.axis_size("lat"), lax.axis_size("lat"))
    return {"lon": lon_at, "lat": lat_at}


def greet(places):
    barrier = pltpu.get_barrier_semaphore()
    for place in places:
        pl.semaphore_signal(barrier, inc=1, device_id=place, device_id_type=pl.DeviceIdType.MESH)
    pl.semaphore_wait(barrier, len(places))


def remote(src, dst, send, recv, place):
    return pltpu.make_async_remote_copy(
        src_ref=src, dst_ref=dst, send_sem=send, recv_sem=recv,
        device_id=place, device_id_type=pl.DeviceIdType.MESH,
    )


def halo_kernel(air, up, table, east, north, corner, bias, send, recv):
    greet([spot(-1, 0), spot(0, -1), spot(-1, -1), spot(1, 0), spot(0, 1), spot(1, 1)])
    copies = []
    for n, src in enumerate((air, up)):
        rim = pl.ds(0, LAT_SHIFT)
        edge = pl.ds(0, EDGE)
        copies += [
            remote(src.at[:, rim], north.at[n], send.at[n, 0], recv.at[n, 0], spot(0, -1)),
            remote(src.at[:, :, edge], east.at[n], send.at[n, 1], recv.at[n, 1], spot(-1, 0)),
            remote(src.at[:, rim, edge], corner.at[n], send.at[n, 2], recv.at[n, 2], spot(-1, -1)),
        ]
    for copy in copies:
        copy.start()
    t_val = table[...]
    t_hi = t_val.astype(BF16)
    t_rest = t_val - t_hi.astype(F32)
    t_mid = t_rest.astype(BF16)
    t_lo = (t_rest - t_mid.astype(F32)).astype(BF16)
    for lon_i in range(WLON):
        sel = selection(lon_i)
        b = mm(t_hi, sel) + mm(t_mid, sel) + mm(t_lo, sel)
        bias[:, lon_i, :] = b
    for copy in copies:
        copy.wait()


def halo_call(air, up, table):
    lev, rows, cols, width = air.shape
    spec = pl.BlockSpec(memory_space=pltpu.VMEM)
    return pl.pallas_call(
        halo_kernel,
        out_shape=(
            jax.ShapeDtypeStruct((2, lev, rows, EDGE, width), BF16),
            jax.ShapeDtypeStruct((2, lev, LAT_SHIFT, cols, width), BF16),
            jax.ShapeDtypeStruct((2, lev, LAT_SHIFT, EDGE, width), BF16),
            jax.ShapeDtypeStruct((table.shape[0], WLON, WIN), F32),
        ),
        in_specs=[spec] * 3,
        out_specs=(spec,) * 4,
        scratch_shapes=[pltpu.SemaphoreType.DMA((2, 3)), pltpu.SemaphoreType.DMA((2, 3))],
        compiler_params=pltpu.CompilerParams(
            collective_id=0, has_side_effects=True, vmem_limit_bytes=16 * 1024 * 1024
        ),
        name="halo_in",
    )(air, up, table)


def finish_kernel(
    lons, lats, air, up, out24, out8, grads, table,
    block_out, d_state, d_gain, d_wqkv, d_wproj, d_table,
    got_n, got_e, got_c, land_w, land_t, land_lat, all_w, all_t, land_g,
    h_send, h_recv, w_send, w_recv, t_send, t_recv, l_send, l_recv, gw_send, gw_recv, gt_send, gt_recv, g_send, g_recv,
):
    me, me_lat = lax.axis_index("lon"), lax.axis_index("lat")
    rows, width = air.shape[1], air.shape[3]
    keep = rows - LAT_SHIFT
    greet(
        [spot(k, 0) for k in range(1, lons)]
        + [spot(0, k) for k in range(1, lats)]
        + [spot(1, 1), spot(-1, -1)]
    )
    w_copies, t_copies = [], []
    for k in range(1, lons):
        to = spot(k, 0)
        w_copies.append(remote(grads.at[to["lon"]], land_w.at[k - 1], w_send.at[k - 1], w_recv.at[k - 1], to))
        t_copies.append(remote(table.at[to["lon"]], land_t.at[me], t_send.at[k - 1], t_recv.at[k - 1], to))
    rim = pl.ds(keep, LAT_SHIFT)
    own = pl.ds(0, keep)
    halos = [
        remote(out24.at[:, :, rim], got_n, h_send.at[0], h_recv.at[0], spot(0, 1)),
        remote(out8.at[:, :, own], got_e, h_send.at[1], h_recv.at[1], spot(1, 0)),
        remote(out8.at[:, :, rim], got_c, h_send.at[2], h_recv.at[2], spot(1, 1)),
    ]
    for copy in w_copies + halos + t_copies:
        copy.start()

    total = grads[me].astype(F32)
    for k in range(1, lons):
        w_copies[k - 1].wait_recv()
        total = total + land_w[k - 1].astype(F32)
    land_lat[me_lat] = total.astype(BF16)
    l_copies = [
        remote(land_lat.at[me_lat], land_lat.at[me_lat], l_send.at[k - 1], l_recv.at[k - 1], spot(0, k))
        for k in range(1, lats)
    ]
    for copy in l_copies:
        copy.start()

    land_t[me] = table[me]
    for k in range(1, lons):
        t_copies[k - 1].wait_recv()
    total = land_t[0].astype(F32)
    for n in range(1, lons):
        total = total + land_t[n].astype(F32)
    t_share = table.shape[1]
    land_g[me_lat] = total[t_share - 8:].astype(BF16)
    g_copies = [
        remote(land_g.at[me_lat], land_g.at[me_lat], g_send.at[k - 1], g_recv.at[k - 1], spot(0, k))
        for k in range(1, lats)
    ]
    for copy in g_copies:
        copy.start()
    all_t[me] = total.astype(BF16)
    gt_copies = [
        remote(all_t.at[me], all_t.at[me], gt_send.at[k - 1], gt_recv.at[k - 1], spot(k, 0))
        for k in range(1, lons)
    ]
    for copy in gt_copies:
        copy.start()

    for copy in halos:
        copy.wait_recv()
    for n, (src, dst) in enumerate(((air, block_out), (up, d_state))):
        for lv in range(air.shape[0]):
            for r in range(rows):
                base = src[lv, r].astype(F32)
                if r < LAT_SHIFT:
                    wide, edge = got_n[n, lv, r], got_c[n, lv, r]
                else:
                    wide, edge = out24[n, lv, r - LAT_SHIFT], got_e[n, lv, r - LAT_SHIFT]
                base = base + wide.astype(F32)
                head = base[:EDGE] + edge.astype(F32)
                dst[lv, r] = jnp.concatenate([head, base[EDGE:]], axis=0).astype(BF16)

    for copy in l_copies:
        copy.wait_recv()
    total = land_lat[0].astype(F32)
    for k in range(1, lats):
        total = total + land_lat[k].astype(F32)
    all_w[me] = total.astype(BF16)
    gw_copies = [
        remote(all_w.at[me], all_w.at[me], gw_send.at[k - 1], gw_recv.at[k - 1], spot(k, 0))
        for k in range(1, lons)
    ]
    for copy in gw_copies:
        copy.start()

    for copy in g_copies:
        copy.wait_recv()
    total = land_g[0].astype(F32)
    for k in range(1, lats):
        total = total + land_g[k].astype(F32)
    d_gain[...] = total[:, 0:width]
    for copy in gt_copies:
        copy.wait_recv()
    d_table[...] = all_t[:, 0:d_table.shape[1]].astype(F32)
    for copy in gw_copies:
        copy.wait_recv()
    d_wqkv[...] = all_w[:, :, 0:3 * width].astype(F32)
    d_wproj[...] = all_w[:, :, 3 * width:4 * width].astype(F32)
    for copy in w_copies + t_copies + halos + l_copies + gt_copies + gw_copies + g_copies:
        copy.wait_send()


def finish_call(air, up, out24, out8, grads, table, lats, t_per):
    lev, rows, cols, width = air.shape
    lons, share, wide = grads.shape
    spec = pl.BlockSpec(memory_space=pltpu.VMEM)
    dma = pltpu.SemaphoreType.DMA
    per = width // lons
    return pl.pallas_call(
        partial(finish_kernel, lons, lats),
        out_shape=(
            jax.ShapeDtypeStruct(air.shape, BF16),
            jax.ShapeDtypeStruct(air.shape, BF16),
            jax.ShapeDtypeStruct((8, width), F32),
            jax.ShapeDtypeStruct((lons, per, 3 * width), F32),
            jax.ShapeDtypeStruct((lons, per, width), F32),
            jax.ShapeDtypeStruct((lons, t_per, table.shape[2]), F32),
        ),
        in_specs=[spec] * 6,
        out_specs=(spec,) * 6,
        scratch_shapes=[
            pltpu.VMEM((2, lev, LAT_SHIFT, cols, width), BF16),
            pltpu.VMEM((2, lev, rows - LAT_SHIFT, EDGE, width), BF16),
            pltpu.VMEM((2, lev, LAT_SHIFT, EDGE, width), BF16),
            pltpu.VMEM((lons - 1, share, wide), BF16),
            pltpu.VMEM(table.shape, BF16),
            pltpu.VMEM((lats, share, wide), BF16),
            pltpu.VMEM(grads.shape, BF16),
            pltpu.VMEM(table.shape, BF16),
            pltpu.VMEM((lats, 8, table.shape[2]), BF16),
            dma((3,)), dma((3,)),
            dma((lons - 1,)), dma((lons - 1,)),
            dma((lons - 1,)), dma((lons - 1,)),
            dma((lats - 1,)), dma((lats - 1,)),
            dma((lons - 1,)), dma((lons - 1,)),
            dma((lons - 1,)), dma((lons - 1,)),
            dma((lats - 1,)), dma((lats - 1,)),
        ],
        compiler_params=pltpu.CompilerParams(
            collective_id=1, has_side_effects=True, vmem_limit_bytes=20 * 1024 * 1024
        ),
        name="finish",
    )(air, up, out24, out8, grads, table)


def on_device(air_state, upstream, norm_gain, w_qkv, w_proj, bias_table):
    lev, rows, cols, width = air_state.shape
    lons, lats = lax.axis_size("lon"), lax.axis_size("lat")
    pairs = (lev // WLEV) * HEADS
    table = bias_table.reshape(pairs * PLACES, PLACES * OFFS)
    east, north, corner, bias = halo_call(air_state, upstream, table)
    out24, out8, grads, d_table = core_call(
        air_state, upstream, east, north, corner, norm_gain.reshape(1, width), w_qkv, w_proj,
        bias, lons,
    )
    block_out, d_state, d_gain, d_wqkv, d_wproj, d_table = finish_call(
        air_state, upstream, out24, out8, grads, d_table, lats, pairs * PLACES // lons
    )
    return (
        block_out, d_state, d_gain[7], d_wqkv.reshape(width, 3 * width), d_wproj.reshape(width, width),
        d_table.reshape(bias_table.shape),
    )


def solution(mesh):
    return jax.shard_map(
        on_device,
        mesh=mesh,
        in_specs=(
            P(None, "lat", "lon", None),
            P(None, "lat", "lon", None),
            P(),
            P(),
            P(),
            P("lat", None, None, None),
        ),
        out_specs=(
            P(None, "lat", "lon", None),
            P(None, "lat", "lon", None),
            P(),
            P(),
            P(),
            P("lat", None, None, None),
        ),
        check_vma=False,
    )
```
